32 devices in a mesh: fsdp: 8 (over z, x), grp: 4 (over y, core).
Axes of the slice: x: 2, y: 2, z: 4, core: 2. Of those that a mesh axis runs over, the one named last changes fastest.
Arguments:
- gradient: bfloat16 [24, 512, 512], P('fsdp', 'grp'), may hold values from -6 to 6
- left_factor: bfloat16 [96, 512, 512], P(('fsdp', 'grp'))
- right_factor: bfloat16 [96, 512, 512], P(('fsdp', 'grp'))
- block_owner: int32 [24], replicated, may hold values from 0 to 31, as said below
Outputs:
- preconditioned: bfloat16 [24, 512, 512], P('fsdp', 'grp')
The draws below stay inside these ranges and needn't reach their ends.
Inputs may be any that keep to these rules, and one draw needn't show every extreme that they name: block_owner[b] is a device index, fsdp index times 4 plus grp index. The 3 blocks homed at one fsdp index go to devices of 3 different fsdp indices; the devices of each fsdp index own 3 blocks in all; no device owns more than 3 blocks, and at every fsdp index one device owns exactly 3.
All inputs are finite; a program needn't handle non-finite values.
Results may differ from the reference program's by a relative error of at most 0.0049.
Values may be sent and summed in bfloat16 or wider, within the bound.
A program may use at most 64 MiB of HBM per device.

```python
import jax
import jax.numpy as jnp
from jax import lax

B = 512
CAP = 3
BLOCKS_COL = 3
BLOCKS = 24
N_FSDP = 8
N_GRP = 4


def draw_factor_common(key, salt_value):
    key_diag, key_noise = jax.random.split(jax.random.fold_in(key, salt_value))
    count = N_FSDP * N_GRP * CAP
    diagonal = jax.random.uniform(key_diag, (count, B), jnp.float32, 0.5, 1.5)
    noise = jax.random.normal(key_noise, (count, B, B), jnp.float32) * (0.5 / B ** 0.5)
    identity = jnp.eye(B, dtype=jnp.float32)
    return noise + diagonal[:, :, None] * identity[None, :, :]


def draw_left_factor(key, part):
    return draw_factor_common(key, 21).astype(jnp.bfloat16)


def draw_right_factor(key, part):
    return draw_factor_common(key, 37).astype(jnp.bfloat16)


def draw_block_owner(key, part):
    key_offsets, key_full, key_order = jax.random.split(jax.random.fold_in(key, 11), 3)
    offsets = jax.random.permutation(key_offsets, N_FSDP)[:BLOCKS_COL].astype(jnp.int32)
    halfway = N_FSDP // 2
    has_half = jnp.any(offsets == halfway)
    offsets = offsets.at[0].set(jnp.where(has_half, offsets[0], halfway)).astype(jnp.int32)
    column_ids = jnp.arange(N_FSDP, dtype=jnp.int32)
    dest_column = (column_ids[:, None] + offsets[None, :]) % N_FSDP
    source_column = (column_ids[:, None] - offsets[None, :]) % N_FSDP
    arrival_rank = jnp.sum(source_column[:, None, :] < source_column[:, :, None], axis=2).astype(jnp.int32)
    full_owner = jax.random.randint(key_full, (N_FSDP,), 0, N_GRP)
    spare_slots = N_GRP * CAP - CAP
    priority = jax.random.randint(key_order, (N_FSDP, spare_slots), 0, 1 << 20) * spare_slots + jnp.arange(spare_slots, dtype=jnp.int32)[None, :]
    spare_order = jnp.argsort(priority, axis=1).astype(jnp.int32)
    later_owner = jnp.take_along_axis(spare_order, jnp.clip(arrival_rank - CAP, 0, spare_slots - 1), axis=1) // CAP
    later_owner = later_owner + (later_owner >= full_owner[:, None]).astype(jnp.int32)
    owner_group = jnp.where(arrival_rank < CAP, full_owner[:, None], later_owner)
    picked = owner_group[dest_column, jnp.arange(BLOCKS_COL, dtype=jnp.int32)[None, :]]
    return (dest_column * N_GRP + picked).reshape(-1).astype(jnp.int32)


def shard_levels(rng, shape, cuts, low, top_value):
    def one(axis_at, shards_of):
        heights = jax.random.uniform(jax.random.fold_in(jax.random.fold_in(rng, 6), axis_at), (shards_of,), jnp.float32, low / len(cuts), top_value / len(cuts))
        return jnp.repeat(jnp.exp(heights), shape[axis_at] // shards_of).reshape((-1,) + (1,) * (len(shape) - axis_at - 1))

    level = one(*cuts[0])
    for cut in cuts[1:]:
        level = level * one(*cut)
    return level


def bell_draw(own_key, extent, spread, limit, cuts=(), held_as=jnp.bfloat16):
    entries = jax.random.normal(own_key, extent, jnp.float32) * spread
    if len(cuts) > 0:
        entries = shard_levels(own_key, extent, cuts, -0.22, 0.18) * entries
    return jnp.clip(entries, min=-limit, max=limit).astype(held_as)


def setup_inputs(seed: int = 0) -> dict:
    streams_of = jax.random.split(jax.random.key(seed), 5)
    return {
        "gradient": bell_draw(streams_of[0], (BLOCKS, B, B), 1.0, 6.0, ((0, 8), (1, 4))),
        "left_factor": draw_left_factor(jax.random.fold_in(streams_of[4], 71), 0),
        "right_factor": draw_right_factor(jax.random.fold_in(streams_of[4], 71), 0),
        "block_owner": draw_block_owner(jax.random.fold_in(streams_of[4], 71), 0),
    }


def reference(gradient, left_factor, right_factor, block_owner):
    block_ids = jnp.arange(BLOCKS, dtype=jnp.int32)
    earlier = (block_owner[None, :] == block_owner[:, None]) & (block_ids[None, :] < block_ids[:, None])
    slot_index = (block_owner + 0).astype(jnp.int32) * CAP + jnp.sum(earlier, axis=1).astype(jnp.int32)

    def precondition_group(packed):
        grad_group, indices = packed
        left_group = jnp.take(left_factor, indices, axis=0).astype(jnp.float32)
        right_group = jnp.take(right_factor, indices, axis=0).astype(jnp.float32)
        product = jnp.einsum("kab,kbc->kac", left_group, grad_group.astype(jnp.float32)).astype(jnp.bfloat16)
        return jnp.einsum("kab,kbc->kac", product.astype(jnp.float32), right_group).astype(jnp.bfloat16)

    grouped = gradient.reshape(BLOCKS // BLOCKS_COL, BLOCKS_COL, B, B)
    indices_grouped = slot_index.reshape(BLOCKS // BLOCKS_COL, BLOCKS_COL).astype(jnp.int32)
    stacked = lax.map(precondition_group, (grouped, indices_grouped))
    return stacked.reshape(BLOCKS, B, B)
```

```python
import functools

import jax
import jax.numpy as jnp
from jax import lax
from jax.experimental import pallas as pl
from jax.experimental.pallas import tpu as pltpu
from jax.sharding import PartitionSpec as P

MESH = pl.DeviceIdType.MESH
CHUNKS = 4


def per_device(gradient, left_factor, right_factor, block_owner):
    local_blocks = gradient.shape[0]
    piece_rows = gradient.shape[1]
    block_width = gradient.shape[2]
    slot_count = left_factor.shape[0]
    columns = lax.axis_size("fsdp")
    groups = lax.axis_size("grp")
    column = lax.axis_index("fsdp")
    owners_all = block_owner.reshape(columns, local_blocks)
    dest_column = owners_all // groups
    dest_group = owners_all % groups
    mine_column = lax.dynamic_index_in_dim(dest_column, column, 0, keepdims=False)
    column_ids = jnp.arange(columns, dtype=jnp.int32)
    matching = mine_column[None, :] == column_ids[:, None]
    pick_send = matching.astype(jnp.bfloat16)
    outgoing = jnp.einsum(
        "cj,jrd->crd", pick_send, gradient, preferred_element_type=jnp.float32
    ).astype(jnp.bfloat16)
    arrived = lax.all_to_all(
        outgoing.reshape(columns * piece_rows, block_width),
        "fsdp",
        split_axis=0,
        concat_axis=0,
        tiled=True,
    )
    arrived = arrived.reshape(columns, piece_rows, block_width)
    toward = dest_column == column
    live_source = jnp.sum(toward.astype(jnp.int32), axis=1) > 0
    target = jnp.sum(jnp.where(toward, dest_group, 0), axis=1)
    same_owner = (target[None, :] == target[:, None]) & live_source[None, :] & live_source[:, None]
    before = column_ids[None, :] < column_ids[:, None]
    rank_slot = jnp.sum((same_owner & before).astype(jnp.int32), axis=1)
    group_ids = jnp.arange(groups, dtype=jnp.int32)
    slot_ids = jnp.arange(slot_count, dtype=jnp.int32)
    routing = (
        live_source[None, None, :]
        & (target[None, None, :] == group_ids[:, None, None])
        & (rank_slot[None, None, :] == slot_ids[None, :, None])
    )
    routing = routing.astype(jnp.bfloat16)
    packed = jnp.einsum(
        "oks,srd->kord", routing, arrived, preferred_element_type=jnp.float32
    ).astype(jnp.bfloat16)
    packed = packed.reshape(slot_count, groups * piece_rows, block_width)
    blocks = lax.all_to_all(packed, "grp", split_axis=1, concat_axis=1, tiled=True)
    left_product = jnp.einsum(
        "kab,kbc->kac", left_factor, blocks, preferred_element_type=jnp.float32
    ).astype(jnp.bfloat16)
    result = jnp.einsum(
        "kab,kbc->kac", left_product, right_factor, preferred_element_type=jnp.float32
    ).astype(jnp.bfloat16)
    returned = lax.all_to_all(result, "grp", split_axis=1, concat_axis=1, tiled=True)
    returned = returned.reshape(slot_count, groups, piece_rows, block_width)
    unpacked = jnp.einsum(
        "oks,kord->srd", routing, returned, preferred_element_type=jnp.float32
    ).astype(jnp.bfloat16)
    homeward = lax.all_to_all(
        unpacked.reshape(columns * piece_rows, block_width),
        "fsdp",
        split_axis=0,
        concat_axis=0,
        tiled=True,
    )
    homeward = homeward.reshape(columns, piece_rows, block_width)
    return jnp.einsum(
        "cj,crd->jrd", pick_send, homeward, preferred_element_type=jnp.float32
    ).astype(jnp.bfloat16)


def preconditioner_kernel(
    columns, groups, blocks, rows, width, chunks,
    owner_ref, g_hbm, l_hbm, r_hbm, out_ref,
    gv, lv, rv, snd, gf, lp, pc, rcvc, sely, rcvy, snd2, *rest,
):
    arr = rest[:chunks]
    res = rest[chunks:2 * chunks]
    arr2 = rest[2 * chunks:3 * chunks]
    (load_sem, fs_s, fs_r, y_s, y_r, c_s, c_r,
     rc_s, rc_r, ry_s, ry_r, hs_s, hs_r) = rest[3 * chunks:]
    col = lax.axis_index("fsdp")
    grp = lax.axis_index("grp")
    core = grp % 2
    half = grp // 2
    mate = half * 2 + (1 - core)
    across = (1 - half) * 2 + core
    w = width // chunks

    loads = [
        pltpu.make_async_copy(g_hbm, gv, load_sem.at[0]),
        pltpu.make_async_copy(l_hbm, lv, load_sem.at[1]),
        pltpu.make_async_copy(r_hbm, rv, load_sem.at[2]),
    ]
    for load in loads:
        load.start()

    barrier = pltpu.get_barrier_semaphore()
    for s in range(1, columns):
        pl.semaphore_signal(barrier, inc=1, device_id={"fsdp": (col + s) % columns}, device_id_type=MESH)
    pl.semaphore_signal(barrier, inc=1, device_id={"grp": mate}, device_id_type=MESH)
    pl.semaphore_signal(barrier, inc=1, device_id={"grp": across}, device_id_type=MESH)

    mine = [owner_ref[col * blocks + j] for j in range(blocks)]
    my_dest = [m // groups for m in mine]
    zero = jnp.int32(0)
    rank_of = []
    source = [zero] * blocks
    count = zero
    owner_group = zero
    for s in range(columns):
        rank_of.append(jnp.minimum(count, blocks - 1))
        live = zero
        for j in range(blocks):
            o = owner_ref[s * blocks + j]
            hit = (o // groups) == col
            live = jnp.where(hit, 1, live)
            owner_group = jnp.where(hit, o % groups, owner_group)
        for k in range(blocks):
            source[k] = jnp.where((live == 1) & (count == k), s, source[k])
        count = count + live
    owner_core = owner_group % 2
    owner_half = owner_group // 2

    def block_for(d):
        j_d = zero
        for j in range(1, blocks):
            j_d = jnp.where(my_dest[j] == d, j, j_d)
        return j_d

    def rank_for(d):
        k_d = zero
        for s in range(columns):
            k_d = jnp.where(d == s, rank_of[s], k_d)
        return k_d

    order = list(range(1, columns))
    peers = {s: (col + s) % columns for s in order}
    senders = {s: (col + columns - s) % columns for s in order}

    def exchange(buf, into, q, s, send_sems, recv_sems):
        return pltpu.make_async_remote_copy(
            src_ref=buf.at[q, s], dst_ref=into[q].at[col],
            send_sem=send_sems.at[q, s], recv_sem=recv_sems.at[q, s],
            device_id={"fsdp": peers[s]}, device_id_type=MESH,
        )

    def arrival(buf, into, q, s, send_sems, recv_sems):
        return pltpu.make_async_remote_copy(
            src_ref=buf.at[q, s], dst_ref=into[q].at[senders[s]],
            send_sem=send_sems.at[q, s], recv_sem=recv_sems.at[q, s],
            device_id={"fsdp": peers[s]}, device_id_type=MESH,
        )

    def to_group(src, dst, send_sem, recv_sem, g):
        return pltpu.make_async_remote_copy(
            src_ref=src, dst_ref=dst, send_sem=send_sem, recv_sem=recv_sem,
            device_id={"grp": g}, device_id_type=MESH,
        )

    loads[0].wait()
    blocks_to = {s: block_for(peers[s]) for s in order}
    own_block = block_for(col)
    for q in range(chunks):
        for s in order:
            snd[q, s] = gv[blocks_to[s], :, q * w:(q + 1) * w]
        arr[q][col] = gv[own_block, :, q * w:(q + 1) * w]
    pl.semaphore_wait(barrier, columns + 1)
    pending = []
    for q in range(chunks):
        for s in order:
            c = exchange(snd, arr, q, s, fs_s, fs_r)
            c.start()
            pending.append(c)
    loads[1].wait()
    loads[2].wait()

    for q in range(chunks):
        for s in order:
            arrival(snd, arr, q, s, fs_s, fs_r).wait_recv()
        for k in range(blocks):
            gf[q, grp, k] = arr[q][source[k]]
        first = to_group(gf.at[q, grp], gf.at[q, grp], y_s.at[q], y_r.at[q], across)
        first.start()
        direct = to_group(gf.at[q, grp], gf.at[q, grp], c_s.at[q, 0], c_r.at[q, 0], mate)
        direct.start()
        to_group(gf.at[q, across], gf.at[q, across], y_s.at[q], y_r.at[q], across).wait_recv()
        onward = to_group(gf.at[q, across], gf.at[q, across], c_s.at[q, 1], c_r.at[q, 1], mate)
        onward.start()
        pending += [first, direct, onward]
        diagonal = (1 - half) * 2 + (1 - core)
        to_group(gf.at[q, mate], gf.at[q, mate], c_s.at[q, 0], c_r.at[q, 0], mate).wait_recv()
        to_group(gf.at[q, diagonal], gf.at[q, diagonal], c_s.at[q, 1], c_r.at[q, 1], mate).wait_recv()
        for k in range(blocks):
            g_cols = gf[q, :, k].reshape(groups * rows, w)
            lp[k, :, q * w:(q + 1) * w] = jnp.dot(
                lv[k], g_cols, preferred_element_type=jnp.float32
            ).astype(jnp.bfloat16)

    for q in range(chunks):
        for k in range(blocks):
            p = jnp.dot(
                lp[k], rv[k, :, q * w:(q + 1) * w], preferred_element_type=jnp.float32
            ).astype(jnp.bfloat16)
            for g in range(groups):
                pc[q, g % 2, g // 2, k] = p[g * rows:(g + 1) * rows]
        c = to_group(pc.at[q, 1 - core], rcvc.at[q], rc_s.at[q], rc_r.at[q], mate)
        c.start()
        pending.append(c)

    def forward_rows(q):
        to_group(pc.at[q, 1 - core], rcvc.at[q], rc_s.at[q], rc_r.at[q], mate).wait_recv()
        sely[q] = jnp.where(owner_core == core, pc[q, core, 1 - half], rcvc[q, 1 - half])
        c = to_group(sely.at[q], rcvy.at[q], ry_s.at[q], ry_r.at[q], across)
        c.start()
        return c

    for q in range(chunks):
        pending.append(forward_rows(q))
    ranks = {s: rank_for(peers[s]) for s in order}
    own_rank = rank_for(col)
    for q in range(chunks):
        to_group(sely.at[q], rcvy.at[q], ry_s.at[q], ry_r.at[q], across).wait_recv()
        near = jnp.where(owner_core == core, pc[q, core, half], rcvc[q, half])
        res[q][...] = jnp.where(owner_half == half, near, rcvy[q])
        for s in order:
            snd2[q, s] = res[q][ranks[s]]
            c = exchange(snd2, arr2, q, s, hs_s, hs_r)
            c.start()
            pending.append(c)
        arr2[q][col] = res[q][own_rank]
    for q in range(chunks):
        for s in order:
            arrival(snd2, arr2, q, s, hs_s, hs_r).wait_recv()
        for j in range(blocks):
            out_ref[j, :, q * w:(q + 1) * w] = arr2[q][my_dest[j]]
    for c in pending:
        c.wait_send()


def per_device_fused(gradient, left_factor, right_factor, block_owner):
    blocks, rows, width = gradient.shape
    columns = lax.axis_size("fsdp")
    groups = lax.axis_size("grp")
    q = CHUNKS
    w = width // q
    bf = jnp.bfloat16
    dma = pltpu.SemaphoreType.DMA
    piece = pltpu.VMEM((columns, rows, w), bf)
    return pl.pallas_call(
        functools.partial(preconditioner_kernel, columns, groups, blocks, rows, width, q),
        out_shape=jax.ShapeDtypeStruct(gradient.shape, gradient.dtype),
        in_specs=[pl.BlockSpec(memory_space=pltpu.SMEM)] + [pl.BlockSpec(memory_space=pl.ANY)] * 3,
        out_specs=pl.BlockSpec(memory_space=pltpu.VMEM),
        scratch_shapes=[
            pltpu.VMEM(gradient.shape, bf),
            pltpu.VMEM(left_factor.shape, bf),
            pltpu.VMEM(right_factor.shape, bf),
            pltpu.VMEM((q, columns, rows, w), bf),
            pltpu.VMEM((q, groups, blocks, rows, w), bf),
            pltpu.VMEM((blocks, width, width), bf),
            pltpu.VMEM((q, 2, 2, blocks, rows, w), bf),
            pltpu.VMEM((q, 2, blocks, rows, w), bf),
            pltpu.VMEM((q, blocks, rows, w), bf),
            pltpu.VMEM((q, blocks, rows, w), bf),
            pltpu.VMEM((q, columns, rows, w), bf),
        ]
        + [piece] * q
        + [pltpu.VMEM((blocks, rows, w), bf)] * q
        + [piece] * q
        + [
            dma((3,)),
            dma((q, columns)), dma((q, columns)),
            dma((q,)), dma((q,)),
            dma((q, 2)), dma((q, 2)),
            dma((q,)), dma((q,)),
            dma((q,)), dma((q,)),
            dma((q, columns)), dma((q, columns)),
        ],
        compiler_params=pltpu.CompilerParams(
            collective_id=0, has_side_effects=True, vmem_limit_bytes=48 * 1024 * 1024
        ),
    )(block_owner, gradient, left_factor, right_factor)


def per_device_any(gradient, left_factor, right_factor, block_owner):
    blocks = gradient.shape[0]
    fits = (
        blocks == left_factor.shape[0]
        and lax.axis_size("grp") == 4
        and gradient.shape[2] % (CHUNKS * 128) == 0
    )
    body = per_device_fused if fits else per_device
    return body(gradient, left_factor, right_factor, block_owner)


def solution(mesh):
    return jax.shard_map(
        per_device_any,
        mesh=mesh,
        in_specs=(
            P("fsdp", "grp", None),
            P(("fsdp", "grp"), None, None),
            P(("fsdp", "grp"), None, None),
            P(),
        ),
        out_specs=P("fsdp", "grp", None),
        check_vma=False,
    )
```

```python
import functools

import jax
import jax.numpy as jnp
from jax import lax
from jax.experimental import pallas as pl
from jax.experimental.pallas import tpu as pltpu
from jax.sharding import PartitionSpec as P

MESH = pl.DeviceIdType.MESH
CHUNKS = 4
SPLITS = 1


def per_device(gradient, left_factor, right_factor, block_owner):
    local_blocks = gradient.shape[0]
    piece_rows = gradient.shape[1]
    block_width = gradient.shape[2]
    slot_count = left_factor.shape[0]
    columns = lax.axis_size("fsdp")
    groups = lax.axis_size("grp")
    column = lax.axis_index("fsdp")
    owners_all = block_owner.reshape(columns, local_blocks)
    dest_column = owners_all // groups
    dest_group = owners_all % groups
    mine_column = lax.dynamic_index_in_dim(dest_column, column, 0, keepdims=False)
    column_ids = jnp.arange(columns, dtype=jnp.int32)
    matching = mine_column[None, :] == column_ids[:, None]
    pick_send = matching.astype(jnp.bfloat16)
    outgoing = jnp.einsum(
        "cj,jrd->crd", pick_send, gradient, preferred_element_type=jnp.float32
    ).astype(jnp.bfloat16)
    arrived = lax.all_to_all(
        outgoing.reshape(columns * piece_rows, block_width),
        "fsdp",
        split_axis=0,
        concat_axis=0,
        tiled=True,
    )
    arrived = arrived.reshape(columns, piece_rows, block_width)
    toward = dest_column == column
    live_source = jnp.sum(toward.astype(jnp.int32), axis=1) > 0
    target = jnp.sum(jnp.where(toward, dest_group, 0), axis=1)
    same_owner = (target[None, :] == target[:, None]) & live_source[None, :] & live_source[:, None]
    before = column_ids[None, :] < column_ids[:, None]
    rank_slot = jnp.sum((same_owner & before).astype(jnp.int32), axis=1)
    group_ids = jnp.arange(groups, dtype=jnp.int32)
    slot_ids = jnp.arange(slot_count, dtype=jnp.int32)
    routing = (
        live_source[None, None, :]
        & (target[None, None, :] == group_ids[:, None, None])
        & (rank_slot[None, None, :] == slot_ids[None, :, None])
    )
    routing = routing.astype(jnp.bfloat16)
    packed = jnp.einsum(
        "oks,srd->kord", routing, arrived, preferred_element_type=jnp.float32
    ).astype(jnp.bfloat16)
    packed = packed.reshape(slot_count, groups * piece_rows, block_width)
    blocks = lax.all_to_all(packed, "grp", split_axis=1, concat_axis=1, tiled=True)
    left_product = jnp.einsum(
        "kab,kbc->kac", left_factor, blocks, preferred_element_type=jnp.float32
    ).astype(jnp.bfloat16)
    result = jnp.einsum(
        "kab,kbc->kac", left_product, right_factor, preferred_element_type=jnp.float32
    ).astype(jnp.bfloat16)
    returned = lax.all_to_all(result, "grp", split_axis=1, concat_axis=1, tiled=True)
    returned = returned.reshape(slot_count, groups, piece_rows, block_width)
    unpacked = jnp.einsum(
        "oks,kord->srd", routing, returned, preferred_element_type=jnp.float32
    ).astype(jnp.bfloat16)
    homeward = lax.all_to_all(
        unpacked.reshape(columns * piece_rows, block_width),
        "fsdp",
        split_axis=0,
        concat_axis=0,
        tiled=True,
    )
    homeward = homeward.reshape(columns, piece_rows, block_width)
    return jnp.einsum(
        "cj,crd->jrd", pick_send, homeward, preferred_element_type=jnp.float32
    ).astype(jnp.bfloat16)


def preconditioner_kernel(
    columns, groups, blocks, rows, width, chunks, splits,
    owner_ref, g_hbm, l_hbm, r_hbm, out_ref,
    gv, lv, rv, snd, gf, lp, pc, rcvc, sely, rcvy, snd2, *rest,
):
    parts = chunks * splits
    arr = rest[:parts]
    res = rest[parts:2 * parts]
    arr2 = rest[2 * parts:3 * parts]
    (load_sem, fs_s, fs_r, y_s, y_r, c_s, c_r,
     rc_s, rc_r, ry_s, ry_r, hs_s, hs_r) = rest[3 * parts:]
    col = lax.axis_index("fsdp")
    grp = lax.axis_index("grp")
    core = grp % 2
    half = grp // 2
    mate = half * 2 + (1 - core)
    across = (1 - half) * 2 + core
    w = width // chunks
    h = rows // splits

    def cols_of(t):
        return slice((t // splits) * w, (t // splits + 1) * w)

    def rows_of(t):
        return pl.ds((t % splits) * h, h)

    def partner(s):
        d, b = 0, 1
        while b < columns:
            v = (col // b) % 2
            d, b = d + b * ((1 - v) if s & b else v), 2 * b
        return d

    loads = [
        pltpu.make_async_copy(g_hbm, gv, load_sem.at[0]),
        pltpu.make_async_copy(l_hbm, lv, load_sem.at[1]),
        pltpu.make_async_copy(r_hbm, rv, load_sem.at[2]),
    ]
    for load in loads:
        load.start()

    barrier = pltpu.get_barrier_semaphore()
    for s in range(1, columns):
        pl.semaphore_signal(barrier, inc=1, device_id={"fsdp": partner(s)}, device_id_type=MESH)
    pl.semaphore_signal(barrier, inc=1, device_id={"grp": mate}, device_id_type=MESH)
    pl.semaphore_signal(barrier, inc=1, device_id={"grp": across}, device_id_type=MESH)

    mine = [owner_ref[col * blocks + j] for j in range(blocks)]
    my_dest = [m // groups for m in mine]
    zero = jnp.int32(0)
    rank_of = []
    source = [zero] * blocks
    count = zero
    owner_group = zero
    for s in range(columns):
        rank_of.append(jnp.minimum(count, blocks - 1))
        live = zero
        for j in range(blocks):
            o = owner_ref[s * blocks + j]
            hit = (o // groups) == col
            live = jnp.where(hit, 1, live)
            owner_group = jnp.where(hit, o % groups, owner_group)
        for k in range(blocks):
            source[k] = jnp.where((live == 1) & (count == k), s, source[k])
        count = count + live
    owner_core = owner_group % 2
    owner_half = owner_group // 2

    def block_for(d):
        j_d = zero
        for j in range(1, blocks):
            j_d = jnp.where(my_dest[j] == d, j, j_d)
        return j_d

    def rank_for(d):
        k_d = zero
        for s in range(columns):
            k_d = jnp.where(d == s, rank_of[s], k_d)
        return k_d

    order = list(range(columns - 1, 0, -1))
    peers = {s: partner(s) for s in order}

    def exchange(buf, into, q, s, send_sems, recv_sems):
        return pltpu.make_async_remote_copy(
            src_ref=buf.at[q, s], dst_ref=into[q].at[col],
            send_sem=send_sems.at[q, s], recv_sem=recv_sems.at[q, s],
            device_id={"fsdp": peers[s]}, device_id_type=MESH,
        )

    def arrival(buf, into, q, s, send_sems, recv_sems):
        return pltpu.make_async_remote_copy(
            src_ref=buf.at[q, s], dst_ref=into[q].at[peers[s]],
            send_sem=send_sems.at[q, s], recv_sem=recv_sems.at[q, s],
            device_id={"fsdp": peers[s]}, device_id_type=MESH,
        )

    def to_group(src, dst, send_sem, recv_sem, g):
        return pltpu.make_async_remote_copy(
            src_ref=src, dst_ref=dst, send_sem=send_sem, recv_sem=recv_sem,
            device_id={"grp": g}, device_id_type=MESH,
        )

    loads[0].wait()
    blocks_to = {s: block_for(peers[s]) for s in order}
    own_block = block_for(col)
    for t in range(parts):
        for s in order:
            snd[t, s] = gv[blocks_to[s], rows_of(t), cols_of(t)]
        arr[t][col] = gv[own_block, rows_of(t), cols_of(t)]
    pl.semaphore_wait(barrier, columns + 1)
    pending = []
    for t in range(parts):
        for s in order:
            c = exchange(snd, arr, t, s, fs_s, fs_r)
            c.start()
            pending.append(c)
    loads[1].wait()
    loads[2].wait()

    def gathered(t, g):
        return gf.at[t // splits, g, :, rows_of(t)]

    def across_copy(t, g):
        return to_group(gathered(t, g), gathered(t, g), y_s.at[t], y_r.at[t], across)

    def mate_copy(t, g, i):
        return to_group(gathered(t, g), gathered(t, g), c_s.at[t, i], c_r.at[t, i], mate)

    diagonal = (1 - half) * 2 + (1 - core)

    def take_in(t):
        for s in order:
            arrival(snd, arr, t, s, fs_s, fs_r).wait_recv()
        for k in range(blocks):
            gf[t // splits, grp, k, rows_of(t)] = arr[t][source[k]]
        first = across_copy(t, grp)
        first.start()
        direct = mate_copy(t, grp, 0)
        direct.start()
        pending.extend([first, direct])

    def pass_on(t):
        across_copy(t, across).wait_recv()
        onward = mate_copy(t, across, 1)
        onward.start()
        pending.append(onward)

    def left(q):
        for t in range(q * splits, (q + 1) * splits):
            mate_copy(t, mate, 0).wait_recv()
            mate_copy(t, diagonal, 1).wait_recv()
        for k in range(blocks):
            g_cols = gf[q, :, k].reshape(groups * rows, w)
            lp[k, :, q * w:(q + 1) * w] = jnp.dot(
                lv[k], g_cols, preferred_element_type=jnp.float32
            ).astype(jnp.bfloat16)

    for t in range(parts):
        take_in(t)
        if t > 0:
            pass_on(t - 1)
            if t % splits == 0:
                left(t // splits - 1)
    pass_on(parts - 1)
    left(chunks - 1)

    def home_copy(q):
        return to_group(pc.at[q, 1 - core], rcvc.at[q], rc_s.at[q], rc_r.at[q], mate)

    def right(q):
        for k in range(blocks):
            p = jnp.dot(
                lp[k], rv[k, :, q * w:(q + 1) * w], preferred_element_type=jnp.float32
            ).astype(jnp.bfloat16)
            for g in range(groups):
                pc[q, g % 2, g // 2, k] = p[g * rows:(g + 1) * rows]
        c = home_copy(q)
        c.start()
        pending.append(c)

    def back_copy(t):
        return to_group(sely.at[t], rcvy.at[t], ry_s.at[t], ry_r.at[t], across)

    def forward_rows(q):
        home_copy(q).wait_recv()
        for t in range(q * splits, (q + 1) * splits):
            r = rows_of(t)
            sely[t] = jnp.where(
                owner_core == core, pc[q, core, 1 - half, :, r], rcvc[q, 1 - half, :, r]
            )
            c = back_copy(t)
            c.start()
            pending.append(c)

    ranks = {s: rank_for(peers[s]) for s in order}
    own_rank = rank_for(col)

    def send_home(t):
        q, r = t // splits, rows_of(t)
        back_copy(t).wait_recv()
        near = jnp.where(owner_core == core, pc[q, core, half, :, r], rcvc[q, half, :, r])
        res[t][...] = jnp.where(owner_half == half, near, rcvy[t])
        for s in order:
            snd2[t, s] = res[t][ranks[s]]
            c = exchange(snd2, arr2, t, s, hs_s, hs_r)
            c.start()
            pending.append(c)
        arr2[t][col] = res[t][own_rank]

    for q in range(chunks):
        right(q)
        if q > 0:
            forward_rows(q - 1)
        if q > 1:
            send_home((q - 2) * splits)
    forward_rows(chunks - 1)
    for t in range(parts):
        if t % splits or t // splits > chunks - 3:
            send_home(t)

    for t in range(parts):
        for s in order:
            arrival(snd2, arr2, t, s, hs_s, hs_r).wait_recv()
        for j in range(blocks):
            out_ref[j, rows_of(t), cols_of(t)] = arr2[t][my_dest[j]]
    for c in pending:
        c.wait_send()


def per_device_fused(gradient, left_factor, right_factor, block_owner):
    blocks, rows, width = gradient.shape
    columns = lax.axis_size("fsdp")
    groups = lax.axis_size("grp")
    q, splits = CHUNKS, SPLITS
    t = q * splits
    w = width // q
    h = rows // splits
    bf = jnp.bfloat16
    dma = pltpu.SemaphoreType.DMA
    piece = pltpu.VMEM((columns, h, w), bf)
    return pl.pallas_call(
        functools.partial(preconditioner_kernel, columns, groups, blocks, rows, width, q, splits),
        out_shape=jax.ShapeDtypeStruct(gradient.shape, gradient.dtype),
        in_specs=[pl.BlockSpec(memory_space=pltpu.SMEM)] + [pl.BlockSpec(memory_space=pl.ANY)] * 3,
        out_specs=pl.BlockSpec(memory_space=pltpu.VMEM),
        scratch_shapes=[
            pltpu.VMEM(gradient.shape, bf),
            pltpu.VMEM(left_factor.shape, bf),
            pltpu.VMEM(right_factor.shape, bf),
            pltpu.VMEM((t, columns, h, w), bf),
            pltpu.VMEM((q, groups, blocks, rows, w), bf),
            pltpu.VMEM((blocks, width, width), bf),
            pltpu.VMEM((q, 2, 2, blocks, rows, w), bf),
            pltpu.VMEM((q, 2, blocks, rows, w), bf),
            pltpu.VMEM((t, blocks, h, w), bf),
            pltpu.VMEM((t, blocks, h, w), bf),
            pltpu.VMEM((t, columns, h, w), bf),
        ]
        + [piece] * t
        + [pltpu.VMEM((blocks, h, w), bf)] * t
        + [piece] * t
        + [
            dma((3,)),
            dma((t, columns)), dma((t, columns)),
            dma((t,)), dma((t,)),
            dma((t, 2)), dma((t, 2)),
            dma((q,)), dma((q,)),
            dma((t,)), dma((t,)),
            dma((t, columns)), dma((t, columns)),
        ],
        compiler_params=pltpu.CompilerParams(
            collective_id=0, has_side_effects=True, vmem_limit_bytes=67043328
        ),
    )(block_owner, gradient, left_factor, right_factor)


def per_device_any(gradient, left_factor, right_factor, block_owner):
    blocks = gradient.shape[0]
    fits = (
        blocks == left_factor.shape[0]
        and lax.axis_size("grp") == 4
        and lax.axis_size("fsdp") & (lax.axis_size("fsdp") - 1) == 0
        and gradient.shape[1] % (SPLITS * 16) == 0
        and gradient.shape[2] % (CHUNKS * 128) == 0
    )
    body = per_device_fused if fits else per_device
    return body(gradient, left_factor, right_factor, block_owner)


def solution(mesh):
    return jax.shard_map(
        per_device_any,
        mesh=mesh,
        in_specs=(
            P("fsdp", "grp", None),
            P(("fsdp", "grp"), None, None),
            P(("fsdp", "grp"), None, None),
            P(),
        ),
        out_specs=P("fsdp", "grp", None),
        check_vma=False,
    )
```

```python
import functools

import jax
import jax.numpy as jnp
from jax import lax
from jax.experimental import pallas as pl
from jax.experimental.pallas import tpu as pltpu
from jax.sharding import PartitionSpec as P

MESH = pl.DeviceIdType.MESH
CHUNKS = 4
WINDOW = 2


def per_device(gradient, left_factor, right_factor, block_owner):
    local_blocks = gradient.shape[0]
    piece_rows = gradient.shape[1]
    block_width = gradient.shape[2]
    slot_count = left_factor.shape[0]
    columns = lax.axis_size("fsdp")
    groups = lax.axis_size("grp")
    column = lax.axis_index("fsdp")
    owners_all = block_owner.reshape(columns, local_blocks)
    dest_column = owners_all // groups
    dest_group = owners_all % groups
    mine_column = lax.dynamic_index_in_dim(dest_column, column, 0, keepdims=False)
    column_ids = jnp.arange(columns, dtype=jnp.int32)
    matching = mine_column[None, :] == column_ids[:, None]
    pick_send = matching.astype(jnp.bfloat16)
    outgoing = jnp.einsum(
        "cj,jrd->crd", pick_send, gradient, preferred_element_type=jnp.float32
    ).astype(jnp.bfloat16)
    arrived = lax.all_to_all(
        outgoing.reshape(columns * piece_rows, block_width),
        "fsdp",
        split_axis=0,
        concat_axis=0,
        tiled=True,
    )
    arrived = arrived.reshape(columns, piece_rows, block_width)
    toward = dest_column == column
    live_source = jnp.sum(toward.astype(jnp.int32), axis=1) > 0
    target = jnp.sum(jnp.where(toward, dest_group, 0), axis=1)
    same_owner = (target[None, :] == target[:, None]) & live_source[None, :] & live_source[:, None]
    before = column_ids[None, :] < column_ids[:, None]
    rank_slot = jnp.sum((same_owner & before).astype(jnp.int32), axis=1)
    group_ids = jnp.arange(groups, dtype=jnp.int32)
    slot_ids = jnp.arange(slot_count, dtype=jnp.int32)
    routing = (
        live_source[None, None, :]
        & (target[None, None, :] == group_ids[:, None, None])
        & (rank_slot[None, None, :] == slot_ids[None, :, None])
    )
    routing = routing.astype(jnp.bfloat16)
    packed = jnp.einsum(
        "oks,srd->kord", routing, arrived, preferred_element_type=jnp.float32
    ).astype(jnp.bfloat16)
    packed = packed.reshape(slot_count, groups * piece_rows, block_width)
    blocks = lax.all_to_all(packed, "grp", split_axis=1, concat_axis=1, tiled=True)
    left_product = jnp.einsum(
        "kab,kbc->kac", left_factor, blocks, preferred_element_type=jnp.float32
    ).astype(jnp.bfloat16)
    result = jnp.einsum(
        "kab,kbc->kac", left_product, right_factor, preferred_element_type=jnp.float32
    ).astype(jnp.bfloat16)
    returned = lax.all_to_all(result, "grp", split_axis=1, concat_axis=1, tiled=True)
    returned = returned.reshape(slot_count, groups, piece_rows, block_width)
    unpacked = jnp.einsum(
        "oks,kord->srd", routing, returned, preferred_element_type=jnp.float32
    ).astype(jnp.bfloat16)
    homeward = lax.all_to_all(
        unpacked.reshape(columns * piece_rows, block_width),
        "fsdp",
        split_axis=0,
        concat_axis=0,
        tiled=True,
    )
    homeward = homeward.reshape(columns, piece_rows, block_width)
    return jnp.einsum(
        "cj,crd->jrd", pick_send, homeward, preferred_element_type=jnp.float32
    ).astype(jnp.bfloat16)


def preconditioner_kernel(
    columns, groups, blocks, rows, width, chunks, teams,
    owner_ref, g_hbm, l_hbm, r_hbm, out_ref, gv, lv, rv, load_sem, *rest,
):
    rest = list(rest)
    room = [dict() for _ in teams]
    for each in room:
        for name in ("snd", "gf", "lp", "pc", "rcvc", "sely", "rcvy", "snd2"):
            each[name] = rest.pop(0)
        for name in ("arr", "res", "arr2"):
            each[name] = [rest.pop(0) for _ in range(chunks)]
        for name in ("out", "across", "mate", "home", "back", "ret"):
            each[name] = (rest.pop(0), rest.pop(0))
    col = lax.axis_index("fsdp")
    grp = lax.axis_index("grp")
    core = grp % 2
    half = grp // 2
    mate = half * 2 + (1 - core)
    across = (1 - half) * 2 + core
    diagonal = (1 - half) * 2 + (1 - core)
    w = width // chunks

    def cols_of(q):
        return slice(q * w, (q + 1) * w)

    def partner(s):
        d, b = 0, 1
        while b < columns:
            v = (col // b) % 2
            d, b = d + b * ((1 - v) if s & b else v), 2 * b
        return d

    loads = [
        pltpu.make_async_copy(g_hbm, gv, load_sem.at[0]),
        pltpu.make_async_copy(l_hbm, lv, load_sem.at[1]),
        pltpu.make_async_copy(r_hbm, rv, load_sem.at[2]),
    ]
    for load in loads:
        load.start()

    peers = [partner(s) for s in range(columns)]
    barrier = pltpu.get_barrier_semaphore()
    for s in range(1, columns):
        pl.semaphore_signal(barrier, inc=1, device_id={"fsdp": peers[s]}, device_id_type=MESH)
    pl.semaphore_signal(barrier, inc=1, device_id={"grp": mate}, device_id_type=MESH)
    pl.semaphore_signal(barrier, inc=1, device_id={"grp": across}, device_id_type=MESH)

    zero = jnp.int32(0)
    my_dest = [owner_ref[col * blocks + j] // groups for j in range(blocks)]
    rank_of = []
    live_of = []
    count = zero
    owner_group = zero
    for c in range(columns):
        live = zero
        for j in range(blocks):
            o = owner_ref[c * blocks + j]
            hit = (o // groups) == col
            live = jnp.where(hit, 1, live)
            owner_group = jnp.where(hit, o % groups, owner_group)
        rank_of.append(jnp.minimum(count, blocks - 1))
        live_of.append(live)
        count = count + live
    owner_core = owner_group % 2
    owner_half = owner_group // 2

    def look_up(table, index):
        found = zero
        for n, value in enumerate(table):
            found = jnp.where(index == n, value, found)
        return found

    def block_for(d):
        j_d = zero
        for j in range(1, blocks):
            j_d = jnp.where(my_dest[j] == d, j, j_d)
        return j_d

    plan = []
    for team, each in zip(teams, room):
        size = min(blocks, len(team))
        entry = [zero] * size
        slot = [zero] * size
        place = []
        filled = zero
        for i, s in enumerate(team):
            live = look_up(live_of, peers[s])
            rank = look_up(rank_of, peers[s])
            for p in range(size):
                take = (live == 1) & (filled == p)
                entry[p] = jnp.where(take, i, entry[p])
                slot[p] = jnp.where(take, rank, slot[p])
            place.append(jnp.minimum(filled, size - 1))
            filled = filled + live
        at_home = []
        for j in range(blocks):
            inside, index = zero, zero
            for i, s in enumerate(team):
                hit = my_dest[j] == peers[s]
                inside = jnp.where(hit, 1, inside)
                index = jnp.where(hit, i, index)
            at_home.append((inside, index))
        plan.append((size, entry, slot, place, at_home))

    pending = []

    def launch(copy):
        copy.start()
        pending.append(copy)

    def exchange(a, src, dst, way, q, i):
        sems = room[a][way]
        return pltpu.make_async_remote_copy(
            src_ref=room[a][src].at[q, i], dst_ref=room[a][dst][q].at[i],
            send_sem=sems[0].at[q, i], recv_sem=sems[1].at[q, i],
            device_id={"fsdp": peers[teams[a][i]]}, device_id_type=MESH,
        )

    def to_group(src, dst, sems, index, g):
        return pltpu.make_async_remote_copy(
            src_ref=src, dst_ref=dst,
            send_sem=sems[0].at[index], recv_sem=sems[1].at[index],
            device_id={"grp": g}, device_id_type=MESH,
        )

    def across_copy(a, q, g):
        piece = room[a]["gf"].at[q, g]
        return to_group(piece, piece, room[a]["across"], (q,), across)

    def mate_copy(a, q, g, i):
        piece = room[a]["gf"].at[q, g]
        return to_group(piece, piece, room[a]["mate"], (q, i), mate)

    def home_copy(a, q):
        return to_group(
            room[a]["pc"].at[q, 1 - core], room[a]["rcvc"].at[q], room[a]["home"], (q,), mate
        )

    def back_copy(a, q):
        return to_group(room[a]["sely"].at[q], room[a]["rcvy"].at[q], room[a]["back"], (q,), across)

    def pack(a, q):
        for i, s in enumerate(teams[a]):
            piece = gv[block_for(peers[s]), :, cols_of(q)]
            if s:
                room[a]["snd"][q, i] = piece
            else:
                room[a]["arr"][q][i] = piece

    def send_out(a, q):
        for i, s in enumerate(teams[a]):
            if s:
                launch(exchange(a, "snd", "arr", "out", q, i))

    def take_in(a, q):
        for i, s in enumerate(teams[a]):
            if s:
                exchange(a, "snd", "arr", "out", q, i).wait_recv()
        for b, r in queue[a * chunks + q + WINDOW:a * chunks + q + WINDOW + 1]:
            send_out(b, r)
        size, entry = plan[a][:2]
        for p in range(size):
            room[a]["gf"][q, grp, p] = room[a]["arr"][q][entry[p]]
        launch(across_copy(a, q, grp))
        launch(mate_copy(a, q, grp, 0))

    def pass_on(a, q):
        across_copy(a, q, across).wait_recv()
        launch(mate_copy(a, q, across, 1))

    def left(a, q):
        mate_copy(a, q, mate, 0).wait_recv()
        mate_copy(a, q, diagonal, 1).wait_recv()
        size, _, slot = plan[a][:3]
        for p in range(size):
            g_cols = room[a]["gf"][q, :, p].reshape(groups * rows, w)
            room[a]["lp"][p, :, cols_of(q)] = jnp.dot(
                lv[slot[p]], g_cols, preferred_element_type=jnp.float32
            ).astype(jnp.bfloat16)

    def right(a, q):
        size, _, slot = plan[a][:3]
        for p in range(size):
            product = jnp.dot(
                room[a]["lp"][p], rv[slot[p], :, cols_of(q)], preferred_element_type=jnp.float32
            ).astype(jnp.bfloat16)
            for g in range(groups):
                room[a]["pc"][q, g % 2, g // 2, p] = product[g * rows:(g + 1) * rows]
        launch(home_copy(a, q))

    def owner_side(a, q, which):
        return jnp.where(owner_core == core, room[a]["pc"][q, core, which], room[a]["rcvc"][q, which])

    def forward_rows(a, q):
        home_copy(a, q).wait_recv()
        room[a]["sely"][q] = owner_side(a, q, 1 - half)
        launch(back_copy(a, q))

    def send_home(a, q):
        back_copy(a, q).wait_recv()
        res = room[a]["res"][q]
        res[...] = jnp.where(owner_half == half, owner_side(a, q, half), room[a]["rcvy"][q])
        place = plan[a][3]
        for i, s in enumerate(teams[a]):
            if s:
                room[a]["snd2"][q, i] = res[place[i]]
                launch(exchange(a, "snd2", "arr2", "ret", q, i))
            else:
                room[a]["arr2"][q][i] = res[place[i]]

    loads[0].wait()
    for q in range(chunks):
        pack(0, q)
    pl.semaphore_wait(barrier, columns + 1)
    queue = [(a, q) for a in range(len(teams)) for q in range(chunks)]
    for a, q in queue[:WINDOW]:
        send_out(a, q)
    for q in range(chunks):
        pack(1, q)
    loads[1].wait()
    loads[2].wait()

    last = chunks - 1
    def take_back(a, q):
        for i, s in enumerate(teams[a]):
            if s:
                exchange(a, "snd2", "arr2", "ret", q, i).wait_recv()

    def take_in_next(a, q):
        take_in(a, q)
        if q > 0:
            pass_on(a, q - 1)
            left(a, q - 1)

    def finish(a):
        pass_on(a, last)
        left(a, last)

    def rights(a, start, stop):
        for q in range(start, stop):
            right(a, q)
            if q > 0:
                forward_rows(a, q - 1)
        if stop == chunks:
            forward_rows(a, last)

    for q in range(chunks):
        take_in_next(0, q)
    finish(0)
    middle = chunks // 2
    take_in_next(1, 0)
    rights(0, 0, middle)
    for q in range(1, chunks):
        take_in_next(1, q)
        if q == 1:
            rights(0, middle, chunks)
        if q >= chunks - 2:
            send_home(0, q - (chunks - 2))
    finish(1)
    right(1, 0)
    for q in range(2, chunks):
        take_back(0, q - 2)
        send_home(0, q)
        rights(1, q - 1, q)
    rights(1, chunks - 1, chunks)
    for q in range(chunks):
        take_back(*((0, chunks - 2 + q) if q < 2 else (1, q - 2)))
        send_home(1, q)
    take_back(1, chunks - 2)
    take_back(1, last)

    for q in range(chunks):
        for j in range(blocks):
            inside, index = plan[0][4][j]
            out_ref[j, :, cols_of(q)] = jnp.where(
                inside == 1, room[0]["arr2"][q][index], room[1]["arr2"][q][plan[1][4][j][1]]
            )
    for copy in pending:
        copy.wait_send()


def per_device_fused(gradient, left_factor, right_factor, block_owner):
    blocks, rows, width = gradient.shape
    columns = lax.axis_size("fsdp")
    groups = lax.axis_size("grp")
    q = CHUNKS
    w = width // q
    bf = gradient.dtype
    dma = pltpu.SemaphoreType.DMA
    early = list(range(columns // 2, columns // 2 + columns // 4))
    late = [s for s in range(columns - 1, -1, -1) if s not in early]
    teams = (early, late)
    scratch = [
        pltpu.VMEM(gradient.shape, bf),
        pltpu.VMEM(left_factor.shape, bf),
        pltpu.VMEM(right_factor.shape, bf),
        dma((3,)),
    ]
    for team in teams:
        n, m = len(team), min(blocks, len(team))
        scratch += [
            pltpu.VMEM((q, n, rows, w), bf),
            pltpu.VMEM((q, groups, m, rows, w), bf),
            pltpu.VMEM((m, width, width), bf),
            pltpu.VMEM((q, 2, 2, m, rows, w), bf),
            pltpu.VMEM((q, 2, m, rows, w), bf),
            pltpu.VMEM((q, m, rows, w), bf),
            pltpu.VMEM((q, m, rows, w), bf),
            pltpu.VMEM((q, n, rows, w), bf),
        ]
        scratch += [pltpu.VMEM((n, rows, w), bf)] * q
        scratch += [pltpu.VMEM((m, rows, w), bf)] * q
        scratch += [pltpu.VMEM((n, rows, w), bf)] * q
        for shape in ((q, n), (q,), (q, 2), (q,), (q,), (q, n)):
            scratch += [dma(shape), dma(shape)]
    return pl.pallas_call(
        functools.partial(
            preconditioner_kernel, columns, groups, blocks, rows, width, q, teams
        ),
        out_shape=jax.ShapeDtypeStruct(gradient.shape, gradient.dtype),
        in_specs=[pl.BlockSpec(memory_space=pltpu.SMEM)] + [pl.BlockSpec(memory_space=pl.ANY)] * 3,
        out_specs=pl.BlockSpec(memory_space=pltpu.VMEM),
        scratch_shapes=scratch,
        compiler_params=pltpu.CompilerParams(
            collective_id=0, has_side_effects=True, vmem_limit_bytes=67043328
        ),
    )(block_owner, gradient, left_factor, right_factor)


def per_device_any(gradient, left_factor, right_factor, block_owner):
    blocks = gradient.shape[0]
    columns = lax.axis_size("fsdp")
    fits = (
        blocks == left_factor.shape[0]
        and lax.axis_size("grp") == 4
        and columns >= 4
        and columns & (columns - 1) == 0
        and gradient.shape[2] % (CHUNKS * 128) == 0
    )
    body = per_device_fused if fits else per_device
    return body(gradient, left_factor, right_factor, block_owner)


def solution(mesh):
    return jax.shard_map(
        per_device_any,
        mesh=mesh,
        in_specs=(
            P("fsdp", "grp", None),
            P(("fsdp", "grp"), None, None),
            P(("fsdp", "grp"), None, None),
            P(),
        ),
        out_specs=P("fsdp", "grp", None),
        check_vma=False,
    )
```

```python
import functools

import jax
import jax.numpy as jnp
from jax import lax
from jax.experimental import pallas as pl
from jax.experimental.pallas import tpu as pltpu
from jax.sharding import PartitionSpec as P

MESH = pl.DeviceIdType.MESH
CHUNKS = 4
WINDOW = 2


def per_device(gradient, left_factor, right_factor, block_owner):
    local_blocks = gradient.shape[0]
    piece_rows = gradient.shape[1]
    block_width = gradient.shape[2]
    slot_count = left_factor.shape[0]
    columns = lax.axis_size("fsdp")
    groups = lax.axis_size("grp")
    column = lax.axis_index("fsdp")
    owners_all = block_owner.reshape(columns, local_blocks)
    dest_column = owners_all // groups
    dest_group = owners_all % groups
    mine_column = lax.dynamic_index_in_dim(dest_column, column, 0, keepdims=False)
    column_ids = jnp.arange(columns, dtype=jnp.int32)
    matching = mine_column[None, :] == column_ids[:, None]
    pick_send = matching.astype(jnp.bfloat16)
    outgoing = jnp.einsum(
        "cj,jrd->crd", pick_send, gradient, preferred_element_type=jnp.float32
    ).astype(jnp.bfloat16)
    arrived = lax.all_to_all(
        outgoing.reshape(columns * piece_rows, block_width),
        "fsdp",
        split_axis=0,
        concat_axis=0,
        tiled=True,
    )
    arrived = arrived.reshape(columns, piece_rows, block_width)
    toward = dest_column == column
    live_source = jnp.sum(toward.astype(jnp.int32), axis=1) > 0
    target = jnp.sum(jnp.where(toward, dest_group, 0), axis=1)
    same_owner = (target[None, :] == target[:, None]) & live_source[None, :] & live_source[:, None]
    before = column_ids[None, :] < column_ids[:, None]
    rank_slot = jnp.sum((same_owner & before).astype(jnp.int32), axis=1)
    group_ids = jnp.arange(groups, dtype=jnp.int32)
    slot_ids = jnp.arange(slot_count, dtype=jnp.int32)
    routing = (
        live_source[None, None, :]
        & (target[None, None, :] == group_ids[:, None, None])
        & (rank_slot[None, None, :] == slot_ids[None, :, None])
    )
    routing = routing.astype(jnp.bfloat16)
    packed = jnp.einsum(
        "oks,srd->kord", routing, arrived, preferred_element_type=jnp.float32
    ).astype(jnp.bfloat16)
    packed = packed.reshape(slot_count, groups * piece_rows, block_width)
    blocks = lax.all_to_all(packed, "grp", split_axis=1, concat_axis=1, tiled=True)
    left_product = jnp.einsum(
        "kab,kbc->kac", left_factor, blocks, preferred_element_type=jnp.float32
    ).astype(jnp.bfloat16)
    result = jnp.einsum(
        "kab,kbc->kac", left_product, right_factor, preferred_element_type=jnp.float32
    ).astype(jnp.bfloat16)
    returned = lax.all_to_all(result, "grp", split_axis=1, concat_axis=1, tiled=True)
    returned = returned.reshape(slot_count, groups, piece_rows, block_width)
    unpacked = jnp.einsum(
        "oks,kord->srd", routing, returned, preferred_element_type=jnp.float32
    ).astype(jnp.bfloat16)
    homeward = lax.all_to_all(
        unpacked.reshape(columns * piece_rows, block_width),
        "fsdp",
        split_axis=0,
        concat_axis=0,
        tiled=True,
    )
    homeward = homeward.reshape(columns, piece_rows, block_width)
    return jnp.einsum(
        "cj,crd->jrd", pick_send, homeward, preferred_element_type=jnp.float32
    ).astype(jnp.bfloat16)


def preconditioner_kernel(
    columns, groups, blocks, rows, width, chunks, teams,
    owner_ref, g_hbm, l_hbm, r_hbm, out_ref, gv, lv, rv, load_sem, *rest,
):
    rest = list(rest)
    room = [dict() for _ in teams]
    for each in room:
        for name in ("snd", "gf", "lp", "pc", "rcvc", "sely", "rcvy", "snd2"):
            each[name] = rest.pop(0)
        for name in ("arr", "res", "arr2"):
            each[name] = [rest.pop(0) for _ in range(chunks)]
        for name in ("out", "across", "mate", "home", "back", "ret"):
            each[name] = (rest.pop(0), rest.pop(0))
    col = lax.axis_index("fsdp")
    grp = lax.axis_index("grp")
    core = grp % 2
    half = grp // 2
    mate = half * 2 + (1 - core)
    across = (1 - half) * 2 + core
    diagonal = (1 - half) * 2 + (1 - core)
    w = width // chunks

    def cols_of(q):
        return slice(q * w, (q + 1) * w)

    def partner(s):
        d, b = 0, 1
        while b < columns:
            v = (col // b) % 2
            d, b = d + b * ((1 - v) if s & b else v), 2 * b
        return d

    loads = [
        pltpu.make_async_copy(g_hbm, gv, load_sem.at[0]),
        pltpu.make_async_copy(l_hbm, lv, load_sem.at[1]),
        pltpu.make_async_copy(r_hbm, rv, load_sem.at[2]),
    ]
    for load in loads:
        load.start()

    peers = [partner(s) for s in range(columns)]
    barrier = pltpu.get_barrier_semaphore()
    for s in range(1, columns):
        pl.semaphore_signal(barrier, inc=1, device_id={"fsdp": peers[s]}, device_id_type=MESH)
    pl.semaphore_signal(barrier, inc=1, device_id={"grp": mate}, device_id_type=MESH)
    pl.semaphore_signal(barrier, inc=1, device_id={"grp": across}, device_id_type=MESH)

    zero = jnp.int32(0)
    my_dest = [owner_ref[col * blocks + j] // groups for j in range(blocks)]
    rank_of = []
    live_of = []
    count = zero
    owner_group = zero
    for c in range(columns):
        live = zero
        for j in range(blocks):
            o = owner_ref[c * blocks + j]
            hit = (o // groups) == col
            live = jnp.where(hit, 1, live)
            owner_group = jnp.where(hit, o % groups, owner_group)
        rank_of.append(jnp.minimum(count, blocks - 1))
        live_of.append(live)
        count = count + live
    owner_core = owner_group % 2
    owner_half = owner_group // 2

    def look_up(table, index):
        found = zero
        for n, value in enumerate(table):
            found = jnp.where(index == n, value, found)
        return found

    def block_for(d):
        j_d = zero
        for j in range(1, blocks):
            j_d = jnp.where(my_dest[j] == d, j, j_d)
        return j_d

    plan = []
    for team, each in zip(teams, room):
        size = min(blocks, len(team))
        entry = [zero] * size
        slot = [zero] * size
        place = []
        filled = zero
        for i, s in enumerate(team):
            live = look_up(live_of, peers[s])
            rank = look_up(rank_of, peers[s])
            for p in range(size):
                take = (live == 1) & (filled == p)
                entry[p] = jnp.where(take, i, entry[p])
                slot[p] = jnp.where(take, rank, slot[p])
            place.append(jnp.minimum(filled, size - 1))
            filled = filled + live
        at_home = []
        for j in range(blocks):
            inside, index = zero, zero
            for i, s in enumerate(team):
                hit = my_dest[j] == peers[s]
                inside = jnp.where(hit, 1, inside)
                index = jnp.where(hit, i, index)
            at_home.append((inside, index))
        plan.append((size, entry, slot, place, at_home))

    pending = []

    def launch(copy):
        copy.start()
        pending.append(copy)

    def exchange(a, src, dst, way, q, i):
        sems = room[a][way]
        return pltpu.make_async_remote_copy(
            src_ref=room[a][src].at[q, i], dst_ref=room[a][dst][q].at[i],
            send_sem=sems[0].at[q, i], recv_sem=sems[1].at[q, i],
            device_id={"fsdp": peers[teams[a][i]]}, device_id_type=MESH,
        )

    def to_group(src, dst, sems, index, g):
        return pltpu.make_async_remote_copy(
            src_ref=src, dst_ref=dst,
            send_sem=sems[0].at[index], recv_sem=sems[1].at[index],
            device_id={"grp": g}, device_id_type=MESH,
        )

    def across_copy(a, q, g):
        piece = room[a]["gf"].at[q, g]
        return to_group(piece, piece, room[a]["across"], (q,), across)

    def mate_copy(a, q, g, i):
        piece = room[a]["gf"].at[q, g]
        return to_group(piece, piece, room[a]["mate"], (q, i), mate)

    def home_copy(a, q):
        return to_group(
            room[a]["pc"].at[q, 1 - core], room[a]["rcvc"].at[q], room[a]["home"], (q,), mate
        )

    def back_copy(a, q):
        return to_group(room[a]["sely"].at[q], room[a]["rcvy"].at[q], room[a]["back"], (q,), across)

    def pack(a, q):
        for i, s in enumerate(teams[a]):
            piece = gv[block_for(peers[s]), :, cols_of(q)]
            if s:
                room[a]["snd"][q, i] = piece
            else:
                room[a]["arr"][q][i] = piece

    def send_out(a, q):
        for i, s in enumerate(teams[a]):
            if s:
                launch(exchange(a, "snd", "arr", "out", q, i))

    def take_in(a, q):
        for i, s in enumerate(teams[a]):
            if s:
                exchange(a, "snd", "arr", "out", q, i).wait_recv()
        for b, r in queue[a * chunks + q + WINDOW:a * chunks + q + WINDOW + 1]:
            send_out(b, r)
        size, entry = plan[a][:2]
        for p in range(size):
            room[a]["gf"][q, grp, p] = room[a]["arr"][q][entry[p]]
        launch(across_copy(a, q, grp))
        launch(mate_copy(a, q, grp, 0))

    def pass_on(a, q):
        across_copy(a, q, across).wait_recv()
        launch(mate_copy(a, q, across, 1))

    def left(a, q):
        mate_copy(a, q, mate, 0).wait_recv()
        mate_copy(a, q, diagonal, 1).wait_recv()
        size, _, slot = plan[a][:3]
        for p in range(size):
            g_cols = room[a]["gf"][q, :, p].reshape(groups * rows, w)
            room[a]["lp"][p, :, cols_of(q)] = jnp.dot(
                lv[slot[p]], g_cols, preferred_element_type=jnp.float32
            ).astype(jnp.bfloat16)

    def right(a, q):
        size, _, slot = plan[a][:3]
        for p in range(size):
            product = jnp.dot(
                room[a]["lp"][p], rv[slot[p], :, cols_of(q)], preferred_element_type=jnp.float32
            ).astype(jnp.bfloat16)
            for g in range(groups):
                room[a]["pc"][q, g % 2, g // 2, p] = product[g * rows:(g + 1) * rows]
        launch(home_copy(a, q))

    def owner_side(a, q, which):
        return jnp.where(owner_core == core, room[a]["pc"][q, core, which], room[a]["rcvc"][q, which])

    def forward_rows(a, q):
        home_copy(a, q).wait_recv()
        room[a]["sely"][q] = owner_side(a, q, 1 - half)
        launch(back_copy(a, q))

    def send_home(a, q):
        back_copy(a, q).wait_recv()
        res = room[a]["res"][q]
        res[...] = jnp.where(owner_half == half, owner_side(a, q, half), room[a]["rcvy"][q])
        place = plan[a][3]
        for i, s in enumerate(teams[a]):
            if s:
                room[a]["snd2"][q, i] = res[place[i]]
                launch(exchange(a, "snd2", "arr2", "ret", q, i))
            else:
                room[a]["arr2"][q][i] = res[place[i]]

    loads[0].wait()
    for q in range(chunks):
        pack(0, q)
    pl.semaphore_wait(barrier, columns + 1)
    queue = [(a, q) for a in range(len(teams)) for q in range(chunks)]
    for a, q in queue[:WINDOW]:
        send_out(a, q)
    for q in range(chunks):
        pack(1, q)
    loads[1].wait()
    loads[2].wait()

    last = chunks - 1
    def take_back(a, q):
        for i, s in enumerate(teams[a]):
            if s:
                exchange(a, "snd2", "arr2", "ret", q, i).wait_recv()

    def take_in_next(a, q):
        take_in(a, q)
        if q > 0:
            pass_on(a, q - 1)
            left(a, q - 1)

    def finish(a):
        pass_on(a, last)
        left(a, last)

    def rights(a, start, stop):
        for q in range(start, stop):
            right(a, q)
            if q > 0:
                forward_rows(a, q - 1)
        if stop == chunks:
            forward_rows(a, last)

    for q in range(chunks):
        take_in_next(0, q)
    finish(0)
    middle = chunks // 2
    take_in_next(1, 0)
    rights(0, 0, middle)
    for q in range(1, chunks):
        take_in_next(1, q)
        if q == 1:
            rights(0, middle, chunks)
        if q >= chunks - 2:
            send_home(0, q - (chunks - 2))
    finish(1)
    right(1, 0)
    for q in range(2, chunks):
        take_back(0, q - 2)
        send_home(0, q)
        rights(1, q - 1, q)
    rights(1, chunks - 1, chunks)
    for q in range(chunks):
        take_back(*((0, chunks - 2 + q) if q < 2 else (1, q - 2)))
        send_home(1, q)
    take_back(1, chunks - 2)
    take_back(1, last)

    for q in range(chunks):
        for j in range(blocks):
            inside, index = plan[0][4][j]
            out_ref[j, :, cols_of(q)] = jnp.where(
                inside == 1, room[0]["arr2"][q][index], room[1]["arr2"][q][plan[1][4][j][1]]
            )
    for copy in pending:
        copy.wait_send()


def per_device_fused(gradient, left_factor, right_factor, block_owner):
    blocks, rows, width = gradient.shape
    columns = lax.axis_size("fsdp")
    groups = lax.axis_size("grp")
    q = CHUNKS
    w = width // q
    bf = gradient.dtype
    dma = pltpu.SemaphoreType.DMA
    early = [columns // 2, columns - 1]
    late = [s for s in range(columns - 1, -1, -1) if s not in early]
    teams = (early, late)
    scratch = [
        pltpu.VMEM(gradient.shape, bf),
        pltpu.VMEM(left_factor.shape, bf),
        pltpu.VMEM(right_factor.shape, bf),
        dma((3,)),
    ]
    for team in teams:
        n, m = len(team), min(blocks, len(team))
        scratch += [
            pltpu.VMEM((q, n, rows, w), bf),
            pltpu.VMEM((q, groups, m, rows, w), bf),
            pltpu.VMEM((m, width, width), bf),
            pltpu.VMEM((q, 2, 2, m, rows, w), bf),
            pltpu.VMEM((q, 2, m, rows, w), bf),
            pltpu.VMEM((q, m, rows, w), bf),
            pltpu.VMEM((q, m, rows, w), bf),
            pltpu.VMEM((q, n, rows, w), bf),
        ]
        scratch += [pltpu.VMEM((n, rows, w), bf)] * q
        scratch += [pltpu.VMEM((m, rows, w), bf)] * q
        scratch += [pltpu.VMEM((n, rows, w), bf)] * q
        for shape in ((q, n), (q,), (q, 2), (q,), (q,), (q, n)):
            scratch += [dma(shape), dma(shape)]
    return pl.pallas_call(
        functools.partial(
            preconditioner_kernel, columns, groups, blocks, rows, width, q, teams
        ),
        out_shape=jax.ShapeDtypeStruct(gradient.shape, gradient.dtype),
        in_specs=[pl.BlockSpec(memory_space=pltpu.SMEM)] + [pl.BlockSpec(memory_space=pl.ANY)] * 3,
        out_specs=pl.BlockSpec(memory_space=pltpu.VMEM),
        scratch_shapes=scratch,
        compiler_params=pltpu.CompilerParams(
            collective_id=0, has_side_effects=True, vmem_limit_bytes=67043328
        ),
    )(block_owner, gradient, left_factor, right_factor)


def per_device_any(gradient, left_factor, right_factor, block_owner):
    blocks = gradient.shape[0]
    columns = lax.axis_size("fsdp")
    fits = (
        blocks == left_factor.shape[0]
        and lax.axis_size("grp") == 4
        and columns >= 4
        and columns & (columns - 1) == 0
        and gradient.shape[2] % (CHUNKS * 128) == 0
    )
    body = per_device_fused if fits else per_device
    return body(gradient, left_factor, right_factor, block_owner)


def solution(mesh):
    return jax.shard_map(
        per_device_any,
        mesh=mesh,
        in_specs=(
            P("fsdp", "grp", None),
            P(("fsdp", "grp"), None, None),
            P(("fsdp", "grp"), None, None),
            P(),
        ),
        out_specs=P("fsdp", "grp", None),
        check_vma=False,
    )
```
